64 devices in a mesh: dp: 4 (over x, y), ep: 16 (over z, core).
Axes of the slice: x: 2, y: 2, z: 8, core: 2. Of those that a mesh axis runs over, the one named last changes fastest.
The devices are a block of a 4x4x8 slice.
Arguments:
- x: bfloat16 [32768, 4096], P(('dp', 'ep')), parts along dimension 0
- route_idx: int32 [32768, 2], P(('dp', 'ep')), parts along dimension 0
- gates: float32 [32768, 2], P(('dp', 'ep')), parts along dimension 0
- w1: bfloat16 [16, 4096, 1536], P('ep')
- w3: bfloat16 [16, 4096, 1536], P('ep')
- w2: bfloat16 [16, 1536, 4096], P('ep')
Outputs:
- output: bfloat16 [32768, 4096], P(('dp', 'ep')), parts along dimension 0
There are 4 independent parts. The reference program is written for one: setup_inputs(seed, part) draws one part's arguments, and reference() takes and returns one part's arrays. A program takes and returns all parts, laid end to end along the dimension named above; an argument that names none is the same for every part.
All inputs are finite; a program needn't handle non-finite values.
Results may differ from the reference program's by a relative error of at most 0.001.
Values are sent between devices in bfloat16 or wider.
A program may use at most 768 MiB of HBM per device.

```python
import jax
import jax.numpy as jnp
from jax import lax

D = 4096
FF = 1536
TOK = 512
EP = 16

T = EP * TOK
RB = TOK // 2
NB = 2 * T // RB + EP


def build_route(counts, key):
    ks, kp = jax.random.split(key)
    cum = jnp.cumsum(counts, axis=1)
    r = jnp.arange(TOK)
    s0 = jax.vmap(lambda c: jnp.searchsorted(c, r, side='right'))(cum)
    s1 = jnp.roll(s0, -(TOK // 2), axis=1)
    pairs = jnp.stack([s0, s1], axis=-1).astype(jnp.int32)
    swap = jax.random.bernoulli(ks, 0.5, (EP, TOK))
    pairs = jnp.where(swap[:, :, None], pairs[:, :, ::-1], pairs)
    keys = jax.random.split(kp, EP)
    pairs = jax.vmap(lambda k, p: jax.random.permutation(k, p, axis=0))(keys, pairs)
    return pairs.reshape(T, 2)


def setup_inputs(seed: int = 0, part: int = 0) -> dict:
    key = jax.random.fold_in(jax.random.key(seed), part)
    kx, kr, kg, kh, kc = jax.random.split(key, 5)
    kw1, kw3, kw2 = jax.random.split(jax.random.key(seed + 1), 3)
    x = jax.random.normal(kx, (T, D), jnp.float32).astype(jnp.bfloat16)
    dev = jnp.arange(EP)
    perm = jax.random.permutation(kh, EP)
    hot = perm[:3]
    cold = perm[3:]
    extra = jax.random.randint(kc, (EP, TOK // 4 - EP + 3), 0, EP - 3)
    cold_cnt = jnp.ones((EP, EP - 3), jnp.int32).at[dev[:, None], extra].add(1)
    counts = jnp.zeros((EP, EP), jnp.int32).at[:, cold].set(cold_cnt)
    amt = jnp.array([3 * TOK // 8, TOK // 4, TOK // 8], jnp.int32)
    hot_idx = hot[(jnp.arange(3)[None, :] + dev[:, None]) % 3]
    counts = counts.at[dev[:, None], hot_idx].set(jnp.broadcast_to(amt, (EP, 3)))
    route_idx = build_route(counts, kr)
    g0 = jax.random.uniform(kg, (T,), jnp.float32, 0.3, 0.7)
    gates = jnp.stack([g0, 1.0 - g0], axis=1)
    w1 = (jax.random.normal(kw1, (EP, D, FF), jnp.float32) * D ** -0.5).astype(jnp.bfloat16)
    w3 = (jax.random.normal(kw3, (EP, D, FF), jnp.float32) * D ** -0.5).astype(jnp.bfloat16)
    w2 = (jax.random.normal(kw2, (EP, FF, D), jnp.float32) * FF ** -0.5).astype(jnp.bfloat16)
    return {'x': x, 'route_idx': route_idx, 'gates': gates, 'w1': w1, 'w3': w3, 'w2': w2}


def reference(x, route_idx, gates, w1, w3, w2):
    e = route_idx.reshape(-1)
    g = gates.reshape(-1)
    tk = jnp.arange(2 * T, dtype=jnp.int32) // 2
    order = jnp.argsort(e, stable=True)
    se = e[order]
    counts = jnp.zeros((EP,), jnp.int32).at[e].add(1)
    start = jnp.cumsum(counts) - counts
    padded = (counts + RB - 1) // RB * RB
    pend = jnp.cumsum(padded)
    pstart = pend - padded
    dest = pstart[se] + jnp.arange(2 * T, dtype=jnp.int32) - start[se]
    tbuf = jnp.full((NB * RB,), T, jnp.int32).at[dest].set(tk[order])
    gbufv = jnp.zeros((NB * RB,), jnp.float32).at[dest].set(g[order])
    bexp = jnp.minimum(jnp.searchsorted(pend, jnp.arange(NB) * RB, side='right'), EP - 1)
    xe = jnp.concatenate([x, jnp.zeros((1, D), x.dtype)], axis=0)

    def step(y, blk):
        tb, gb, be = blk
        rows = xe[tb]
        a = jnp.dot(rows, w1[be], preferred_element_type=jnp.float32)
        b = jnp.dot(rows, w3[be], preferred_element_type=jnp.float32)
        h = (jax.nn.silu(a) * b).astype(jnp.bfloat16)
        o = jnp.dot(h, w2[be], preferred_element_type=jnp.float32).astype(jnp.bfloat16)
        return y.at[tb].add(gb[:, None] * o.astype(jnp.float32)), None

    y, _ = lax.scan(step, jnp.zeros((T + 1, D), jnp.float32),
                    (tbuf.reshape(NB, RB), gbufv.reshape(NB, RB), bexp))
    return y[:T].astype(jnp.bfloat16)
```

```python
import jax
import jax.numpy as jnp
from jax import lax
from jax.sharding import PartitionSpec as P

CHUNKS = 4


def ffn(rows, w1, w3, w2):
    a = jnp.dot(rows, w1, preferred_element_type=jnp.float32)
    b = jnp.dot(rows, w3, preferred_element_type=jnp.float32)
    h = (jax.nn.silu(a) * b).astype(jnp.bfloat16)
    return jnp.dot(h, w2, preferred_element_type=jnp.float32).astype(jnp.bfloat16)


def weights(e, g, classes):
    n0 = sum(c[0].astype(jnp.int32) for c in classes)
    n1 = sum(c[1].astype(jnp.int32) for c in classes)
    out = []
    for c0, c1 in classes:
        both = c0 & c1
        pair = (n0 + n1) == 2
        w = jnp.where(c0, jnp.where(pair, g[..., 0], 1.0), 0.0)
        w = w + jnp.where(c1, jnp.where(pair, g[..., 1], 1.0), 0.0)
        out.append(jnp.where(both, 1.0, w))
    return out


def merge(sources, ws):
    total = None
    for v, w in zip(sources, ws):
        w = w[:, None]
        t = jnp.where(w == 0.0, 0.0, w * v.astype(jnp.float32))
        total = t if total is None else total + t
    return total.astype(jnp.bfloat16)


def solution(mesh):
    ep = mesh.shape['ep']
    nz = ep // 2
    far = nz // 2

    def perm_z(step):
        return [(i, (i + 2 * step) % ep) for i in range(ep)]

    swap = [(i, i ^ 1) for i in range(ep)]

    def local(x, route_idx, gates, w1, w3, w2):
        tok, d = x.shape
        n = tok // CHUNKS
        me = lax.axis_index('ep')
        z, c = me // 2, me % 2
        re = lax.all_gather(route_idx, 'ep')
        rg = lax.all_gather(gates, 'ep')
        re = lax.dynamic_index_in_dim(re.reshape(nz, 2, tok, 2), c, 1, keepdims=False)
        rg = lax.dynamic_index_in_dim(rg.reshape(nz, 2, tok, 2), c, 1, keepdims=False)
        home = (z + jnp.arange(nz)) % nz
        re, rg = re[home], rg[home]

        def tables(sign):
            res = []
            for j in range(nz):
                e, g = re[j], rg[j]
                rel = (sign * (home[j] - e // 2)) % nz
                own, par = e == me, e == (me ^ 1)
                r = (sign * j) % nz
                if r == 0:
                    inl = (rel >= 1) & (rel <= far)
                    ins = rel > far
                    cls = [inl, ins, own, par]
                elif r <= far:
                    cls = [(rel > r) & (rel <= far), own, par]
                else:
                    cls = [(rel > far) & (rel < r), own, par]
                res.append(weights(e, g, [(m[:, 0], m[:, 1]) for m in cls]))
            return res

        tabs = {s: tables(s) for s in (1, -1)}
        outs = []
        xs = [lax.all_gather(x[k * n:(k + 1) * n], 'ep') for k in range(CHUNKS)]
        for k in range(CHUNKS):
            sign = 1 if k % 2 == 0 else -1
            tab = tabs[sign]
            sl = slice(k * n, (k + 1) * n)
            o = ffn(xs[k].reshape(ep * n, d), w1[0], w3[0], w2[0]).reshape(nz, 2, n, d)
            own = lax.dynamic_index_in_dim(o, c, 1, keepdims=False)
            par = lax.ppermute(lax.dynamic_index_in_dim(o, 1 - c, 1, keepdims=False), 'ep', swap)

            def at(v, j):
                return lax.dynamic_index_in_dim(v, (z + j) % nz, 0, keepdims=False)

            def walk(first, step):
                msg = None
                for r in range(abs(first), 0, -1):
                    j = (r if first > 0 else -r) % nz
                    w = [t[sl] for t in tab[j]]
                    if msg is None:
                        msg = merge([at(own, j), at(par, j)], w[1:])
                    else:
                        msg = merge([msg, at(own, j), at(par, j)], w)
                    msg = lax.ppermute(msg, 'ep', perm_z(step))
                return msg

            long = walk(sign * far, sign)
            short = walk(-sign * (far - 1), -sign)
            w = [t[sl] for t in tab[0]]
            outs.append(merge([long, short, at(own, 0), at(par, 0)], w))
        return jnp.concatenate(outs, axis=0)

    spec = P(('dp', 'ep'), None)
    wspec = P('ep', None, None)
    return jax.shard_map(local, mesh=mesh, in_specs=(spec, spec, spec, wspec, wspec, wspec),
                         out_specs=spec, check_vma=False)
```

```python
import jax
import jax.numpy as jnp
from jax import lax
from jax.sharding import PartitionSpec as P

PARTS = (12, 18, 20, 14)


def weights(masks, g):
    m = masks.astype(jnp.float32)
    pair = jnp.sum(m, axis=(0, 3), keepdims=True) == 2.0
    w = jnp.sum(m * jnp.where(pair, g[None], 1.0), axis=3, keepdims=True)
    return jnp.where(jnp.sum(m, axis=3, keepdims=True) == 2.0, 1.0, w)


def merge(sources, cols):
    total = None
    for v, (w, empty) in zip(sources, cols):
        t = jnp.where(empty[:, None], 0.0, w[:, None] * v.astype(jnp.float32))
        total = t if total is None else total + t
    return total.astype(jnp.bfloat16)


def solution(mesh):
    ep = mesh.shape['ep']
    nz = ep // 2
    far = nz // 2

    def perm_z(step):
        return [(i, (i + 2 * step) % ep) for i in range(ep)]

    swap = [(i, i ^ 1) for i in range(ep)]

    def local(x, route_idx, gates, w1, w3, w2):
        tok, d = x.shape
        cuts = [tok * sum(PARTS[:k]) // sum(PARTS) for k in range(len(PARTS) + 1)]
        me = lax.axis_index('ep')
        z, c = me // 2, me % 2
        rr = lax.all_gather(jnp.concatenate([route_idx.astype(jnp.float32), gates], axis=1).T, 'ep')
        rr = lax.dynamic_index_in_dim(rr.reshape(nz, 2, 4, tok), c, 1, keepdims=False)
        home = (z + jnp.arange(nz)) % nz
        rr = jnp.take(rr, home, axis=0).transpose(0, 2, 1)
        re, rg = rr[..., :2].astype(jnp.int32), rr[..., 2:]

        def tables(sign):
            rel = (sign * (home[:, None, None] - re // 2)) % nz
            r = ((sign * jnp.arange(nz)) % nz)[:, None, None]
            inl = (rel > r) & (rel <= far) & (r <= far)
            ins = (rel > far) & ((r == 0) | ((r > far) & (rel < r)))
            return weights(jnp.stack([inl, ins, re == me, re == (me ^ 1)]), rg)

        tabs = {1: tables(1), -1: tables(-1)}
        outs = []
        xs = [lax.all_gather(x[lo:hi], 'ep') for lo, hi in zip(cuts, cuts[1:])]
        used = {j: (2, 3) if j == far else (0, 2, 3) if j < far else (1, 2, 3) for j in range(1, nz)}
        used[nz - far + 1] = (2, 3)
        used[0] = (0, 1, 2, 3)
        cols = {}
        for k in range(len(PARTS)):
            sign = 1 if k % 2 == 0 else -1
            for r, sources in used.items():
                for i in sources:
                    w = tabs[sign][i, (sign * r) % nz, cuts[k]:cuts[k + 1], 0]
                    cols[k, (sign * r) % nz, i] = w, w == 0.0
        xs[0], cols = lax.optimization_barrier((xs[0], cols))
        for k in range(len(PARTS)):
            sign = 1 if k % 2 == 0 else -1
            n = cuts[k + 1] - cuts[k]
            rows = xs[k].reshape(ep * n, d)
            a = jnp.dot(rows, w1[0], preferred_element_type=jnp.float32)
            b = jnp.dot(rows, w3[0], preferred_element_type=jnp.float32)
            h = (jax.nn.silu(a) * b).astype(jnp.bfloat16).reshape(nz, 2, n, -1)

            def out(core):
                part = lax.dynamic_index_in_dim(h, core, 1, keepdims=False).reshape(nz * n, -1)
                o = jnp.dot(part, w2[0], preferred_element_type=jnp.float32)
                return o.astype(jnp.bfloat16).reshape(nz, n, d)

            other = out(1 - c)
            par = lax.ppermute(other, 'ep', swap)
            own = out(c)

            def at(v, j):
                return lax.dynamic_index_in_dim(v, (z + j) % nz, 0, keepdims=False)

            def at_place(j, *sources):
                return [cols[k, j, i] for i in sources]

            def walk(first, step, source):
                msg = None
                for r in range(abs(first), 0, -1):
                    j = (r if first > 0 else -r) % nz
                    if msg is None:
                        msg = merge([at(own, j), at(par, j)], at_place(j, 2, 3))
                    else:
                        msg = merge([msg, at(own, j), at(par, j)], at_place(j, source, 2, 3))
                    msg = lax.ppermute(msg, 'ep', perm_z(step))
                return msg

            long = walk(sign * far, sign, 0)
            short = walk(-sign * (far - 1), -sign, 1)
            outs.append(merge([long, short, at(own, 0), at(par, 0)], at_place(0, 0, 1, 2, 3)))
        return jnp.concatenate(outs, axis=0)


    spec = P(('dp', 'ep'), None)
    wspec = P('ep', None, None)
    return jax.shard_map(local, mesh=mesh, in_specs=(spec, spec, spec, wspec, wspec, wspec),
                         out_specs=spec, check_vma=False)
```

```python
import jax
import jax.numpy as jnp
from jax import lax
from jax.sharding import PartitionSpec as P

PARTS = (7, 8, 9, 4, 4)


def weights(masks, g):
    m = masks.astype(jnp.float32)
    pair = jnp.sum(m, axis=(0, 3), keepdims=True) == 2.0
    w = jnp.sum(m * jnp.where(pair, g[None], 1.0), axis=3, keepdims=True)
    return jnp.where(jnp.sum(m, axis=3, keepdims=True) == 2.0, 1.0, w)


def merge(sources, cols):
    total = None
    for v, (w, empty) in zip(sources, cols):
        t = jnp.where(empty[:, None], 0.0, w[:, None] * v.astype(jnp.float32))
        total = t if total is None else total + t
    return total.astype(jnp.bfloat16)


def solution(mesh):
    ep = mesh.shape['ep']
    nz = ep // 2
    far = nz // 2

    def perm_z(step):
        return [(i, (i + 2 * step) % ep) for i in range(ep)]

    swap = [(i, i ^ 1) for i in range(ep)]

    def local(x, route_idx, gates, w1, w3, w2):
        tok, d = x.shape
        cuts = [tok * sum(PARTS[:k]) // sum(PARTS) for k in range(len(PARTS) + 1)]
        me = lax.axis_index('ep')
        z, c = me // 2, me % 2
        rr = lax.all_gather(jnp.concatenate([route_idx.astype(jnp.float32), gates], axis=1).T, 'ep')
        rr = lax.dynamic_index_in_dim(rr.reshape(nz, 2, 4, tok), c, 1, keepdims=False)
        home = (z + jnp.arange(nz)) % nz
        rr = jnp.take(rr, home, axis=0).transpose(0, 2, 1)
        re, rg = rr[..., :2].astype(jnp.int32), rr[..., 2:]

        def tables(sign):
            rel = (sign * (home[:, None, None] - re // 2)) % nz
            r = ((sign * jnp.arange(nz)) % nz)[:, None, None]
            inl = (rel > r) & (rel <= far) & (r <= far)
            ins = (rel > far) & ((r == 0) | ((r > far) & (rel < r)))
            return weights(jnp.stack([inl, ins, re == me, re == (me ^ 1)]), rg)

        tabs = {1: tables(1), -1: tables(-1)}
        outs = []
        xs = []
        for k, (lo, hi) in enumerate(zip(cuts, cuts[1:])):
            xs.append(lax.all_gather(x[lo:hi], 'ep'))
        used = {j: (2, 3) if j == far else (0, 2, 3) if j < far else (1, 2, 3) for j in range(1, nz)}
        used[nz - far + 1] = (2, 3)
        used[0] = (0, 1, 2, 3)
        cols = {}
        for k in range(len(PARTS)):
            sign = 1 if k % 2 == 0 else -1
            for r, sources in used.items():
                for i in sources:
                    w = tabs[sign][i, (sign * r) % nz, cuts[k]:cuts[k + 1], 0]
                    cols[k, (sign * r) % nz, i] = w, w == 0.0
        xs[0], cols = lax.optimization_barrier((xs[0], cols))
        for k in range(len(PARTS)):
            sign = 1 if k % 2 == 0 else -1
            n = cuts[k + 1] - cuts[k]
            rows = xs[k].reshape(ep * n, d)
            a = jnp.dot(rows, w1[0], preferred_element_type=jnp.float32)
            rows, a = lax.optimization_barrier((rows, a))
            b = jnp.dot(rows, w3[0], preferred_element_type=jnp.float32)
            h = (jax.nn.silu(a) * b).astype(jnp.bfloat16).reshape(nz, 2, n, -1)

            def out(h, core):
                part = lax.dynamic_index_in_dim(h, core, 1, keepdims=False).reshape(nz * n, -1)
                o = jnp.dot(part, w2[0], preferred_element_type=jnp.float32)
                return o.astype(jnp.bfloat16).reshape(nz, n, d)

            other = out(h, 1 - c)
            par = lax.ppermute(other, 'ep', swap)
            own = out(lax.optimization_barrier((h, other))[0], c)
            if k + 1 < len(PARTS):
                xs[k + 1] = lax.optimization_barrier((xs[k + 1], own))[0]

            def at(v, j):
                return lax.dynamic_index_in_dim(v, (z + j) % nz, 0, keepdims=False)

            def at_place(j, *sources):
                return [cols[k, j, i] for i in sources]

            def walk(first, step, source):
                msg = None
                for r in range(abs(first), 0, -1):
                    j = (r if first > 0 else -r) % nz
                    if msg is None:
                        msg = merge([at(own, j), at(par, j)], at_place(j, 2, 3))
                    else:
                        msg = merge([msg, at(own, j), at(par, j)], at_place(j, source, 2, 3))
                    msg = lax.ppermute(msg, 'ep', perm_z(step))
                return msg

            long = walk(sign * far, sign, 0)
            short = walk(-sign * (far - 1), -sign, 1)
            outs.append(merge([long, short, at(own, 0), at(par, 0)], at_place(0, 0, 1, 2, 3)))
        return jnp.concatenate(outs, axis=0)

    spec = P(('dp', 'ep'), None)
    wspec = P('ep', None, None)
    return jax.shard_map(local, mesh=mesh, in_specs=(spec, spec, spec, wspec, wspec, wspec),
                         out_specs=spec, check_vma=False)
```
